512 devices in a mesh: dp: 4 (over y), seq: 16 (over z), tensor: 8 (over x, core).
Axes of the slice: x: 4, y: 4, z: 16, core: 2. Of those that a mesh axis runs over, the one named last changes fastest.
Arguments:
- queries: bfloat16 [4, 1024, 8192], P('dp', 'seq', 'tensor'), may hold values from -6 to 6
- new_keys: bfloat16 [4, 1024, 1024], P('dp', 'seq', 'tensor'), may hold values from -6 to 6
- new_values: bfloat16 [4, 1024, 1024], P('dp', 'seq', 'tensor'), may hold values from -6 to 6
- cache_keys: bfloat16 [4, 8192, 1024], P('dp', 'seq', 'tensor'), may hold values from -6 to 6
- cache_values: bfloat16 [4, 8192, 1024], P('dp', 'seq', 'tensor'), may hold values from -6 to 6
- keep_lengths: int32 [4, 16], P('dp', 'seq'), may hold values from 1 to 512
- cache_doc: int32 [4, 8192], P('dp', 'seq'), may hold values from 0 to 1
- new_doc: int32 [4, 1024], P('dp', 'seq'), may hold values from 0 to 1, never falling along the last dimension, each value on 1 to 640 neighbouring positions
- out_weight: bfloat16 [8192, 8192], P('tensor', 'dp'), may hold values from -0.0625 to 0.0625
Outputs:
- mixed_out: bfloat16 [4, 1024, 4, 2048], P('dp', 'seq', None, 'tensor')
The draws below stay inside these ranges and needn't reach their ends.
Inputs may be any that keep to these rules, and one draw needn't show every extreme that they name: `keep_lengths`: valid cache rows of a shard come first. `cache_doc`: documents 0 and 1 of the pack. `new_doc`: never falling along the tokens of a pack; both documents present.
All inputs are finite; a program needn't handle non-finite values.
Results may differ from the reference program's by a relative error of at most 0.0056.
Values may be sent and summed in bfloat16 or wider, within the bound.
No kernel may reach another device: no remote copies, remote signals or barrier semaphores. Data moves between devices by JAX's collectives and lax.ppermute only.
A program may use at most 128 MiB of HBM per device.

```python
import math
import jax
import jax.numpy as jnp
import numpy as np
from jax import lax

D = 8192
HQ = 64
KVH = 8
HD = 128
CACHE_DEV = 512
GROUP = 8
NEW = 1024
PACKS = 4
SHARDS = 16
BLOCKS = 4
COLS = 2048


def base_values(key, width):
    result = jnp.clip(jax.random.normal(key, (PACKS, NEW, width), jnp.float32), -6.0, 6.0)
    return result


def draw_queries(key, part):
    result = base_values(jax.random.fold_in(key, 11), HQ * HD).reshape(PACKS, NEW, HQ, HD)
    return result.reshape(PACKS, NEW, HQ * HD).astype(jnp.bfloat16)


def draw_new_keys(key, part):
    result = base_values(jax.random.fold_in(key, 13), KVH * HD).reshape(PACKS, NEW, KVH, HD)
    return result.reshape(PACKS, NEW, KVH * HD).astype(jnp.bfloat16)


def with_ends(values, rng, least, top_value):
    spot = [jax.random.randint(jax.random.fold_in(rng, axis), (), 0, length) for axis, length in enumerate(values.shape)]
    longest = values.shape.index(max(values.shape))
    neighbour = spot[:longest] + [(spot[longest] + 1) % values.shape[longest]] + spot[longest + 1:]
    return values.at[tuple(spot)].set(least).at[tuple(neighbour)].set(top_value)


def levels(rng, shape, pieces, least, top_value):
    def one(dim, parts):
        heights = jax.random.uniform(jax.random.fold_in(jax.random.fold_in(rng, 6), dim), (parts,), jnp.float32, least / len(pieces), top_value / len(pieces))
        return jnp.repeat(jnp.exp(heights), shape[dim] // parts).reshape((-1,) + (1,) * (len(shape) - dim - 1))

    factor_of = one(*pieces[0])
    for cut in pieces[1:]:
        factor_of = factor_of * one(*cut)
    return factor_of


def profile(count, total, reach, skew):
    weights = [(1 << 20) // math.isqrt(rank ** skew) + 1 for rank in range(2, count + 1)]
    surplus, counts = total - reach - (count - 1), [1] * (count - 1)
    while surplus > 0:
        candidates = [i for i in range(count - 1) if counts[i] < reach]
        pool, remaining = sum([weights[i] for i in candidates]), surplus
        for i in candidates:
            more = min(reach - counts[i], max(1, remaining * weights[i] // pool), surplus)
            counts[i] = counts[i] + more
            surplus = surplus - more
    return np.array([reach] + counts)


def ragged_sizes(own_key, amount, total, reach, lean):
    if amount == 2:
        one = jax.random.randint(own_key, (), max(1, total - reach), min(reach, total - 1) + 1)
        return jnp.stack([one, total - one])
    sizes = jnp.asarray(profile(amount, total, reach, lean), jnp.int32)
    twos = (amount - 1) // 2
    giver, receiver = sizes[1:1 + 2 * twos:2], sizes[2:2 + 2 * twos:2]
    margin = jnp.minimum(giver - 1, reach - receiver)
    shifted = jax.random.randint(jax.random.fold_in(own_key, 1), (twos,), 0, 1 << 20) % (margin + 1)
    sizes = sizes.at[1:1 + 2 * twos:2].set(giver - shifted).at[2:2 + 2 * twos:2].set(receiver + shifted)
    return sizes[jax.random.permutation(jax.random.fold_in(own_key, 2), amount)]


def bell_draw(rng, extent, spread, most, pieces=(), held_as=jnp.bfloat16):
    entries = spread * jax.random.normal(rng, extent, jnp.float32)
    if pieces:
        entries = entries * levels(rng, extent, pieces, -0.22, 0.18)
    return jnp.clip(entries, -most, most).astype(held_as)


def setup_inputs(seed: int = 0) -> dict:
    key_of = jax.random.split(jax.random.key(seed), 10)
    queries = draw_queries(jax.random.fold_in(key_of[9], 71), 0)
    new_keys = draw_new_keys(jax.random.fold_in(key_of[9], 71), 0)
    new_values = bell_draw(key_of[2], (PACKS, NEW, KVH * HD), 1.0, 6.0, ((0, 4), (1, 16), (2, 8)))
    cache_keys = bell_draw(key_of[3], (PACKS, SHARDS * CACHE_DEV, KVH * HD), 1.0, 6.0, ((0, 4), (1, 16), (2, 8)))
    cache_values = bell_draw(key_of[4], (PACKS, SHARDS * CACHE_DEV, KVH * HD), 1.0, 6.0, ((0, 4), (1, 16), (2, 8)))
    keep_lengths = with_ends(jax.random.randint(key_of[5], (PACKS, SHARDS), 1, CACHE_DEV + 1), jax.random.fold_in(key_of[5], 1), 1, CACHE_DEV).astype(jnp.int32)
    cache_doc = with_ends(jax.random.randint(key_of[6], (PACKS, SHARDS * CACHE_DEV), 0, 2), jax.random.fold_in(key_of[6], 1), 0, 1).astype(jnp.int32)
    new_doc = jax.vmap(lambda own: jnp.searchsorted(jnp.cumsum(ragged_sizes(own, 2, NEW, NEW * 5 // 8, 0)), jnp.arange(NEW), side="right"))(jax.random.split(key_of[7], PACKS)).reshape((PACKS, NEW)).astype(jnp.int32)
    out_weight = bell_draw(key_of[8], (HQ * HD, D), (HQ * HD) ** -0.5, 0.0625, ((0, 8), (1, 4)))
    return {"queries": queries, "new_keys": new_keys, "new_values": new_values, "cache_keys": cache_keys, "cache_values": cache_values, "keep_lengths": keep_lengths, "cache_doc": cache_doc, "new_doc": new_doc, "out_weight": out_weight}


masked_score = -1.0e30


def softmax_terms(scores, visible, value_rows):
    scores = jnp.where(visible, scores, masked_score)
    top_score = jnp.max(scores, axis=-1)
    weights = jnp.where(visible, jnp.exp(scores - top_score[..., None]), 0.0)
    weight_sum = jnp.sum(weights, axis=-1)
    summed = jnp.dot(weights.astype(jnp.bfloat16), value_rows, preferred_element_type=jnp.float32)
    return top_score, weight_sum, summed


def reference(queries, new_keys, new_values, cache_keys, cache_values, keep_lengths, cache_doc, new_doc, out_weight):
    score_scale = HD ** -0.5
    row_token = jnp.arange(NEW * GROUP, dtype=jnp.int32) // GROUP
    positions = jnp.arange(CACHE_DEV, dtype=jnp.int32)
    new_index = jnp.arange(NEW, dtype=jnp.int32)
    outputs = []
    for pack_index in range(PACKS):
        query_heads = queries[pack_index].reshape(NEW, KVH, GROUP, HD).transpose(1, 0, 2, 3)
        cache_k = cache_keys[pack_index].reshape(SHARDS, CACHE_DEV, KVH, HD).transpose(2, 0, 1, 3)
        cache_v = cache_values[pack_index].reshape(SHARDS, CACHE_DEV, KVH, HD).transpose(2, 0, 1, 3)
        fresh_k = new_keys[pack_index].reshape(NEW, KVH, HD).transpose(1, 0, 2)
        fresh_v = new_values[pack_index].reshape(NEW, KVH, HD).transpose(1, 0, 2)
        token_doc = new_doc[pack_index]
        row_doc = jnp.repeat(token_doc, GROUP)
        shard_doc = cache_doc[pack_index].reshape(SHARDS, CACHE_DEV)
        lengths = keep_lengths[pack_index]

        def one_head(inputs):
            query_part, key_part, value_part, fresh_keys, fresh_values = inputs
            query_rows = query_part.reshape(NEW * GROUP, HD)

            def one_shard(shard_data):
                key_rows, value_rows, doc_rows, length = shard_data
                scores = jnp.dot(query_rows, key_rows.T, preferred_element_type=jnp.float32) * score_scale
                visible = (positions[None, :] < length) & (doc_rows[None, :] == row_doc[:, None])
                return softmax_terms(scores, visible, value_rows)

            shard_tops, shard_sums, shard_partial = lax.map(one_shard, (key_part, value_part, shard_doc, lengths))
            scores = jnp.dot(query_rows, fresh_keys.T, preferred_element_type=jnp.float32) * score_scale
            visible = (new_index[None, :] <= row_token[:, None]) & (token_doc[None, :] == row_doc[:, None])
            fresh_top, fresh_sum, fresh_partial = softmax_terms(scores, visible, fresh_values)
            all_tops = jnp.concatenate([shard_tops, fresh_top[None]], 0)
            overall_top = jnp.max(all_tops, axis=0)
            factors = jnp.exp(all_tops - overall_top[None])
            denominator = jnp.sum(shard_sums * factors[:-1], 0) + fresh_sum * factors[-1]
            numerator = jnp.sum(shard_partial * factors[:-1, :, None], 0) + fresh_partial * factors[-1][:, None]
            return (numerator / denominator[:, None]).reshape(NEW, GROUP, HD)

        heads_out = lax.map(one_head, (query_heads, cache_k, cache_v, fresh_k, fresh_v))
        attended = heads_out.transpose(1, 0, 2, 3).reshape(NEW, HQ * HD).astype(jnp.bfloat16)
        mixed_out = jnp.dot(attended, out_weight, preferred_element_type=jnp.float32).astype(jnp.bfloat16)
        outputs.append(mixed_out.reshape(NEW, BLOCKS, COLS))
    return jnp.stack(outputs, 0)
```

```python
import math

import jax
import jax.numpy as jnp
from jax import lax
from jax.experimental import pallas as pl
from jax.experimental.pallas import tpu as pltpu
from jax.sharding import Mesh
from jax.sharding import PartitionSpec as P

HD = 128
masked_score = -1e30
to_log2 = 1.4426950408889634


def contract_last(a, b):
    return lax.dot_general(a, b, (((1,), (1,)), ((), ())), preferred_element_type=jnp.float32)


def dot(a, b):
    return lax.dot_general(a, b, (((1,), (0,)), ((), ())), preferred_element_type=jnp.float32)


def lane_tiles(x):
    return [x[:, i : i + HD] for i in range(0, x.shape[1], HD)]


def attend_kernel(sizes, own, last, *refs):
    slots, fresh, groups, chunks = sizes
    place, q_ref, doc_ref, kv_ref = refs[:4]
    refs = refs[4:]
    if own:
        state = None
        outs = refs
    else:
        state = refs[:3]
        outs = refs[3:]
    my = place[0].astype(jnp.float32)
    code_at = 2 * slots + 2 * fresh
    lanes = lax.broadcasted_iota(jnp.int32, (1, HD), 1)
    row_fresh = None
    origin = None
    for c in range(chunks):
        row = kv_ref[c, pl.ds(code_at, 16), :].astype(jnp.float32)
        mine = row[slots // HD : slots // HD + 1]
        start = row[slots // HD + 1 : slots // HD + 2]
        here = (lanes // fresh) == c
        mine = jnp.where(here, mine, -1.0)
        row_fresh = mine if c == 0 else jnp.where(here, mine, row_fresh)
        origin = start if c == 0 else jnp.where(here, start, origin)
    if not own:
        row_fresh = jnp.where(origin < my, row_fresh, -1.0)
    cache_codes = [
        kv_ref[c, pl.ds(code_at, 16), :].astype(jnp.float32)[i : i + 1]
        for c in range(chunks)
        for i in range(slots // HD)
    ]
    fresh_keys = [kv_ref[c, pl.ds(2 * slots, fresh), :] for c in range(chunks)]
    fresh_values = [kv_ref[c, pl.ds(2 * slots + fresh, fresh), :] for c in range(chunks)]
    if chunks == 1:
        blank = jnp.zeros((HD - fresh, HD), jnp.bfloat16)
        fresh_keys.append(blank)
        fresh_values.append(blank)
    fresh_keys = jnp.concatenate(fresh_keys, axis=0)
    fresh_values = jnp.concatenate(fresh_values, axis=0)
    tokens = doc_ref.shape[0]
    block = groups * tokens
    row_doc = jnp.concatenate([doc_ref[...]] * groups, axis=0)
    scale = to_log2 * HD ** (-0.5)

    def body(b, carry):
        at = pl.multiple_of(b * block, block)
        rows = pl.ds(at, block)
        q = q_ref[rows, :]
        tiles = []
        for c in range(chunks):
            tiles += lane_tiles(contract_last(q, kv_ref[c, pl.ds(0, slots), :]))
        tiles = [
            jnp.where(code == row_doc, t * scale, masked_score)
            for t, code in zip(tiles, cache_codes, strict=True)
        ]
        late = contract_last(q, fresh_keys)
        seen = row_fresh == row_doc
        if own:
            token = lax.broadcasted_iota(jnp.int32, (block, HD), 0) % tokens
            k = lax.broadcasted_iota(jnp.int32, (block, HD), 1)
            seen = seen & (k <= token)
        tiles.append(jnp.where(seen, late * scale, masked_score))
        top = tiles[0]
        for t in tiles[1:]:
            top = jnp.maximum(top, t)
        top = jnp.max(top, axis=1, keepdims=True)
        if state is not None:
            before = state[1][rows, :]
            top = jnp.maximum(before, top)
            fade = jnp.exp2(before - top)
        else:
            top = jnp.broadcast_to(top, (block, HD))
        tiles = [jnp.exp2(t - top) for t in tiles]
        total = tiles[0]
        for t in tiles[1:]:
            total = total + t
        weights = [t.astype(jnp.bfloat16) for t in tiles]
        each = slots // HD
        summed = dot(weights[-1], fresh_values)
        for c in range(chunks):
            part = jnp.concatenate(weights[c * each : (c + 1) * each], axis=1)
            summed = summed + dot(part, kv_ref[c, pl.ds(slots, slots), :])
        if state is not None:
            total = total + state[2][rows, :] * fade
            summed = summed + state[0][rows, :] * fade
        if last:
            value = summed / jnp.sum(total, axis=1, keepdims=True)
            value = value.astype(jnp.bfloat16)
            wide = jnp.concatenate([value[g * tokens : (g + 1) * tokens] for g in range(groups)], axis=1)
            width = groups * HD
            for copy in range(outs[0].shape[0]):
                outs[0][copy, :, pl.ds(pl.multiple_of(b * width, width), width)] = wide
        else:
            outs[0][rows, :] = summed
            outs[1][rows, :] = top
            outs[2][rows, :] = total
        return carry

    lax.fori_loop(0, q_ref.shape[0] // block, body, 0)


def attend(place, q, doc, payload, state, slots, fresh, last, copies):
    chunks = payload.shape[0]
    groups = 4
    rows = q.shape[0]
    tokens = doc.shape[0]
    heads = rows // tokens
    own = state is None
    sizes = (slots, fresh, groups, chunks)

    def kernel(*refs):
        attend_kernel(sizes, own, last, *refs)

    if last:
        out_shape = [jax.ShapeDtypeStruct((copies, tokens, heads * HD), jnp.bfloat16)]
    else:
        out_shape = [jax.ShapeDtypeStruct((rows, HD), jnp.float32)] * 3
    args = (place, q, doc, payload, *(() if own else state))
    specs = [pl.BlockSpec(memory_space=pltpu.SMEM)]
    specs += [pl.BlockSpec(memory_space=pltpu.VMEM)] * (len(args) - 1)
    keys = chunks * (slots + fresh)
    return pl.pallas_call(
        kernel,
        out_shape=out_shape,
        in_specs=specs,
        out_specs=[pl.BlockSpec(memory_space=pltpu.VMEM)] * len(out_shape),
        name="attend_last" if last else ("attend_own" if own else "attend_step"),
        cost_estimate=pl.CostEstimate(
            flops=40 * rows * keys * HD,
            bytes_accessed=payload.size * 2 + 6 * rows * HD * 4,
            transcendentals=rows * keys,
        ),
        compiler_params=pltpu.CompilerParams(vmem_limit_bytes=32 * 1024 * 1024),
    )(*args)


def project_kernel(place, a_ref, own_ref, other_ref, out_ref):
    core = place[1]
    packs, each, width = a_ref.shape[0], a_ref.shape[2], a_ref.shape[3]
    mine = a_ref[:, core].reshape(packs * each, width)
    theirs = a_ref[:, 1 - core].reshape(packs * each, width)
    summed = dot(mine, own_ref[...]) + dot(theirs, other_ref[...])
    out_ref[...] = summed.astype(jnp.bfloat16).reshape(packs, 1, each, summed.shape[1])


def project(place, a, own, other, pieces):
    packs, _, each, width = a.shape
    cols = own.shape[1] // pieces
    return pl.pallas_call(
        project_kernel,
        grid=(pieces,),
        out_shape=jax.ShapeDtypeStruct((packs, pieces, each, cols), jnp.bfloat16),
        in_specs=[
            pl.BlockSpec(memory_space=pltpu.SMEM),
            pl.BlockSpec(a.shape, lambda j: (0, 0, 0, 0)),
            pl.BlockSpec((width, cols), lambda j: (0, j)),
            pl.BlockSpec((width, cols), lambda j: (0, j)),
        ],
        out_specs=pl.BlockSpec((packs, 1, each, cols), lambda j: (0, j, 0, 0)),
        name="project",
        cost_estimate=pl.CostEstimate(
            flops=4 * packs * each * width * own.shape[1],
            bytes_accessed=4 * width * own.shape[1],
            transcendentals=0,
        ),
        compiler_params=pltpu.CompilerParams(vmem_limit_bytes=32 * 1024 * 1024),
    )(place, a, own, other)


def swaps(size):
    plans = []
    for shift in (0, 1):
        pairs = []
        for core in (0, 1):
            for s in range(size):
                odd = (s + core + shift) % 2
                pairs.append((s * 2 + core, ((s + (1 if odd == 0 else -1)) % size) * 2 + core))
        plans.append(pairs)
    return plans


def local(
    queries,
    new_keys,
    new_values,
    cache_keys,
    cache_values,
    keep_lengths,
    cache_doc,
    new_doc,
    out_weight,
):
    ring = lax.axis_size("seq")
    packs, mesh_x, cores = lax.axis_size("dp"), lax.axis_size("x"), lax.axis_size("core")
    my = lax.axis_index("seq")
    core = lax.axis_index("core")
    place = jnp.stack([my, core]).astype(jnp.int32)
    fresh = queries.shape[1]
    heads = queries.shape[2] // HD
    slots = cache_keys.shape[1]
    other_weight = lax.ppermute(out_weight, "core", [(0, 1), (1, 0)])

    visible = jnp.arange(slots, dtype=jnp.int32) < keep_lengths[0, 0]
    cache_code = jnp.where(visible, cache_doc[0], -1).astype(jnp.bfloat16).reshape(slots // HD, HD)
    new_code = jnp.tile(new_doc.astype(jnp.bfloat16), (1, HD // fresh))
    origin = jnp.full((1, HD), my, jnp.int32).astype(jnp.bfloat16)
    spare = jnp.zeros((16 - slots // HD - 2, HD), jnp.bfloat16)
    own = jnp.concatenate(
        [cache_keys[0], cache_values[0], new_keys[0], new_values[0], cache_code, new_code, origin, spare],
        axis=0,
    )[None]
    q = queries[0].reshape(fresh, heads, HD).transpose(1, 0, 2).reshape(heads * fresh, HD)
    doc = jnp.broadcast_to(new_doc[0].astype(jnp.float32)[:, None], (fresh, HD))

    plans = swaps(ring)

    def swap(x, step):
        return lax.ppermute(x, ("seq", "core"), plans[step % 2])

    def step(payload, state, last=False):
        return attend(place, q, doc, payload, state, slots, fresh, last, packs)

    steps = ring // 2
    payload = swap(own, 0)
    state = step(own, None)
    arrived = swap(jnp.concatenate([own, payload], axis=0), 1)
    state = step(payload, state)
    for s in range(2, steps):
        payload, arrived = arrived, swap(arrived, s)
        state = step(payload, state)
    (attended,) = step(arrived, state, last=True)

    each = fresh // cores
    tiles = lax.all_to_all(
        attended.reshape(packs * cores, each, heads * HD), ("dp", "core"), 0, 0, tiled=True
    ).reshape(packs, cores, each, heads * HD)
    pieces = project(place, tiles, out_weight, other_weight, mesh_x * cores)
    width = pieces.shape[3]
    arrived = lax.all_to_all(
        pieces.reshape(packs * mesh_x * cores, each, width), ("dp", "x", "core"), 0, 0, tiled=True
    )
    arrived = arrived.reshape(packs, mesh_x, cores, each, width).astype(jnp.float32)
    result = arrived.sum(axis=1).astype(jnp.bfloat16)
    return result.transpose(1, 2, 0, 3).reshape(1, fresh, packs, width)


def solution(mesh):
    shape = dict(mesh.shape)
    cores = 2
    split = Mesh(
        mesh.devices.reshape(shape["dp"], shape["seq"], shape["tensor"] // cores, cores),
        ("dp", "seq", "x", "core"),
    )
    t = ("x", "core")
    placed = (
        P("dp", "seq", t),
        P("dp", "seq", t),
        P("dp", "seq", t),
        P("dp", "seq", t),
        P("dp", "seq", t),
        P("dp", "seq"),
        P("dp", "seq"),
        P("dp", "seq"),
        P(t, "dp"),
    )
    return jax.shard_map(
        local, mesh=split, in_specs=placed, out_specs=P("dp", "seq", None, t), check_vma=False
    )
```

```python
import jax
import jax.numpy as jnp
from jax import lax
from jax.experimental import pallas as pl
from jax.experimental.pallas import tpu as pltpu
from jax.sharding import Mesh
from jax.sharding import PartitionSpec as P


HD = 128
HALVES = 2
CODES = 16
GROUPS = 4
masked_score = -1e30
to_log2 = 1.4426950408889634
VMEM = pl.BlockSpec(memory_space=pltpu.VMEM)
SMEM = pl.BlockSpec(memory_space=pltpu.SMEM)


def contract_last(a, b):
    return lax.dot_general(a, b, (((1,), (1,)), ((), ())), preferred_element_type=jnp.float32)


def dot(a, b):
    return lax.dot_general(a, b, (((1,), (0,)), ((), ())), preferred_element_type=jnp.float32)


def pack_kernel(
    keep_ref, keys, values, new_keys, new_values, doc, new_doc, out_ref, doc_ref, new_doc_ref, sems
):
    slots = keys.shape[0] // HALVES
    fresh = new_keys.shape[0] // HALVES
    copies = [
        pltpu.make_async_copy(doc, doc_ref, sems.at[0]),
        pltpu.make_async_copy(new_doc, new_doc_ref, sems.at[1]),
    ]
    for h in range(HALVES):
        at = 0
        for ref, size in ((keys, slots), (values, slots), (new_keys, fresh), (new_values, fresh)):
            copies.append(
                pltpu.make_async_copy(
                    ref.at[pl.ds(h * size, size)],
                    out_ref.at[h, pl.ds(at, size)],
                    sems.at[len(copies)],
                )
            )
            at += size
    for copy in copies:
        copy.start()
    copies[0].wait()
    copies[1].wait()
    lane = lax.broadcasted_iota(jnp.int32, (1, HD), 1)
    row = lax.broadcasted_iota(jnp.int32, (CODES, HD), 0)
    new_doc = new_doc_ref[...].astype(jnp.float32)
    twice = jnp.concatenate([new_doc] * (HD // new_doc.shape[1]), axis=1)
    turned = pltpu.roll(twice, fresh, 1)
    origin = lax.axis_index("seq").astype(jnp.float32)
    for h in range(HALVES):
        mine = jnp.where((lane // fresh) % HALVES == h, twice, turned)
        codes = jnp.full((CODES, HD), origin, jnp.float32)
        codes = jnp.where(row == slots // HD, mine, codes)
        for i in range(slots // HD):
            first = h * slots + i * HD
            code = doc_ref[:, pl.ds(first, HD)].astype(jnp.float32)
            code = jnp.where(lane + first < keep_ref[0, 0], code, -1.0)
            codes = jnp.where(row == i, code, codes)
        out_ref[h, pl.ds(2 * (slots + fresh), CODES), :] = codes.astype(jnp.bfloat16)
    for copy in copies[2:]:
        copy.wait()


def pack(keep, keys, values, new_keys, new_values, doc, new_doc):
    rows = (keys.shape[0] + values.shape[0] + new_keys.shape[0] + new_values.shape[0]) // HALVES
    return pl.pallas_call(
        pack_kernel,
        out_shape=jax.ShapeDtypeStruct((HALVES, rows + CODES, HD), jnp.bfloat16),
        in_specs=[SMEM] + [pl.BlockSpec(memory_space=pltpu.HBM)] * 6,
        out_specs=VMEM,
        scratch_shapes=[
            pltpu.VMEM(doc.shape, doc.dtype),
            pltpu.VMEM(new_doc.shape, new_doc.dtype),
            pltpu.SemaphoreType.DMA((2 + 4 * HALVES,)),
        ],
        name="pack",
        compiler_params=pltpu.CompilerParams(vmem_limit_bytes=4 * 1024 * 1024),
    )(keep, keys, values, new_keys, new_values, doc, new_doc)


def attend_kernel(own, last, many, *refs):
    queries_ref, doc_ref = refs[:2]
    payloads = refs[2 : 2 + many]
    state = None if own else refs[2 + many : 5 + many]
    outs = refs[2 + many :] if own else refs[5 + many :]
    halves = [(ref, h) for ref in payloads for h in range(ref.shape[0])]
    tokens, width = queries_ref.shape
    fresh = tokens // HALVES
    slots = (payloads[0].shape[1] - CODES - 2 * fresh) // 2
    each = slots // HD
    my = lax.axis_index("seq").astype(jnp.float32)
    lanes = lax.broadcasted_iota(jnp.int32, (1, HD), 1)
    codes = [ref[h, pl.ds(2 * (slots + fresh), CODES), :].astype(jnp.float32) for ref, h in halves]
    cache_codes = [c[i : i + 1] for c in codes for i in range(each)]
    row_fresh = jnp.full((1, HD), -1.0, jnp.float32)
    for n, c in enumerate(codes):
        mine = c[each : each + 1]
        if not own:
            mine = jnp.where(c[each + 1 : each + 2] < my, mine, -1.0)
        row_fresh = jnp.where(lanes // fresh == n, mine, row_fresh)
    new_keys = [ref[h, pl.ds(2 * slots, fresh), :] for ref, h in halves]
    new_values = [ref[h, pl.ds(2 * slots + fresh, fresh), :] for ref, h in halves]
    if len(halves) * fresh < HD:
        blank = jnp.zeros((HD - len(halves) * fresh, HD), jnp.bfloat16)
        new_keys.append(blank)
        new_values.append(blank)
    new_keys = jnp.concatenate(new_keys, axis=0)
    new_values = jnp.concatenate(new_values, axis=0)

    block = GROUPS * tokens
    square = lax.broadcasted_iota(jnp.int32, (tokens, tokens), 0) == lax.broadcasted_iota(
        jnp.int32, (tokens, tokens), 1
    )
    doc = jnp.sum(jnp.where(square, doc_ref[...].astype(jnp.float32), 0.0), axis=1, keepdims=True)
    row_doc = jnp.concatenate([jnp.broadcast_to(doc, (tokens, HD))] * GROUPS, axis=0)
    scale = to_log2 * HD ** (-0.5)

    def body(b, carry):
        rows = pl.ds(pl.multiple_of(b * block, block), block)
        wide = pl.ds(pl.multiple_of(b * GROUPS * HD, GROUPS * HD), GROUPS * HD)
        q = queries_ref[:, wide]
        q = jnp.concatenate([q[:, g * HD : (g + 1) * HD] for g in range(GROUPS)], axis=0)
        tiles = []
        for ref, h in halves:
            scores = contract_last(q, ref[h, pl.ds(0, slots), :])
            tiles += [scores[:, i * HD : (i + 1) * HD] for i in range(each)]
        tiles = [
            jnp.where(code == row_doc, t * scale, masked_score)
            for t, code in zip(tiles, cache_codes, strict=True)
        ]
        late = contract_last(q, new_keys)
        seen = row_fresh == row_doc
        if own:
            token = lax.broadcasted_iota(jnp.int32, (block, HD), 0) % tokens
            seen = seen & (lax.broadcasted_iota(jnp.int32, (block, HD), 1) <= token)
        tiles.append(jnp.where(seen, late * scale, masked_score))
        top = tiles[0]
        for t in tiles[1:]:
            top = jnp.maximum(top, t)
        top = jnp.max(top, axis=1, keepdims=True)
        if own:
            top = jnp.broadcast_to(top, (block, HD))
        else:
            before = state[1][rows, :]
            top = jnp.maximum(before, top)
            fade = jnp.exp2(before - top)
        tiles = [jnp.exp2(t - top) for t in tiles]
        total = tiles[0]
        for t in tiles[1:]:
            total = total + t
        weights = [t.astype(jnp.bfloat16) for t in tiles]
        summed = dot(weights[-1], new_values)
        for n, (ref, h) in enumerate(halves):
            part = jnp.concatenate(weights[n * each : (n + 1) * each], axis=1)
            summed = summed + dot(part, ref[h, pl.ds(slots, slots), :])
        if not own:
            total = total + state[2][rows, :] * fade
            summed = summed + state[0][rows, :] * fade
        if last:
            value = (summed / jnp.sum(total, axis=1, keepdims=True)).astype(jnp.bfloat16)
            value = jnp.concatenate(
                [value[g * tokens : (g + 1) * tokens] for g in range(GROUPS)], axis=1
            )
            for copy in range(outs[0].shape[0]):
                outs[0][copy, :, wide] = value
        else:
            outs[0][rows, :] = summed
            outs[1][rows, :] = top
            outs[2][rows, :] = total
        return carry

    lax.fori_loop(0, width // (GROUPS * HD), body, 0)


def attend(queries, doc, payloads, state, last=0):
    tokens, width = queries.shape
    rows = tokens * width // HD
    own = state is None
    many = len(payloads)

    def kernel(*refs):
        attend_kernel(own, last, many, *refs)

    if last:
        out_shape = [jax.ShapeDtypeStruct((last, tokens, width), jnp.bfloat16)]
    else:
        out_shape = [jax.ShapeDtypeStruct((rows, HD), jnp.float32)] * 3
    args = (queries, doc, *payloads, *(() if own else state))
    keys = sum(p.shape[0] * p.shape[1] for p in payloads) // 2
    return pl.pallas_call(
        kernel,
        out_shape=out_shape,
        in_specs=[VMEM] * len(args),
        out_specs=[VMEM] * len(out_shape),
        name="attend_last" if last else ("attend_own" if own else "attend_step"),
        cost_estimate=pl.CostEstimate(
            flops=16 * rows * keys * HD,
            bytes_accessed=keys * HD * 4 + 6 * rows * HD * 4,
            transcendentals=rows * keys,
        ),
        compiler_params=pltpu.CompilerParams(vmem_limit_bytes=12 * 1024 * 1024),
    )(*args)


def project_kernel(a_ref, own_ref, other_ref, out_ref):
    core = lax.axis_index("core")
    packs, each, width = a_ref.shape[0], a_ref.shape[2], a_ref.shape[3]
    pieces, cols = out_ref.shape[1], out_ref.shape[3]
    mine = a_ref[:, core].reshape(packs * each, width)
    theirs = a_ref[:, 1 - core].reshape(packs * each, width)
    for j in range(pieces):
        at = pl.ds(j * cols, cols)
        summed = dot(mine, own_ref[:, at]) + dot(theirs, other_ref[:, at])
        out_ref[:, j] = summed.astype(jnp.bfloat16).reshape(packs, each, cols)


def project(a, own, other, pieces):
    packs, _, each, width = a.shape
    cols = own.shape[1] // pieces
    block = 2
    return pl.pallas_call(
        project_kernel,
        grid=(pieces // block,),
        out_shape=jax.ShapeDtypeStruct((packs, pieces, each, cols), jnp.bfloat16),
        in_specs=[
            pl.BlockSpec(a.shape, lambda j: (0, 0, 0, 0)),
            pl.BlockSpec((width, cols * block), lambda j: (0, j)),
            pl.BlockSpec((width, cols * block), lambda j: (0, j)),
        ],
        out_specs=pl.BlockSpec((packs, block, each, cols), lambda j: (0, j, 0, 0)),
        name="project",
        cost_estimate=pl.CostEstimate(
            flops=4 * packs * each * width * own.shape[1],
            bytes_accessed=4 * width * own.shape[1],
            transcendentals=0,
        ),
        compiler_params=pltpu.CompilerParams(vmem_limit_bytes=16 * 1024 * 1024),
    )(a, own, other)


def gather_sum_kernel(parts_ref, out_ref):
    packs, terms, cores, each, cols = parts_ref.shape
    for d in range(packs):
        for c in range(cores):
            total = parts_ref[d, 0, c].astype(jnp.float32)
            for t in range(1, terms):
                total = total + parts_ref[d, t, c].astype(jnp.float32)
            out_ref[pl.ds(c * each, each), pl.ds(d * cols, cols)] = total.astype(jnp.bfloat16)


def gather_sum(parts):
    packs, _, cores, each, cols = parts.shape
    return pl.pallas_call(
        gather_sum_kernel,
        out_shape=jax.ShapeDtypeStruct((cores * each, packs * cols), jnp.bfloat16),
        in_specs=[VMEM],
        out_specs=VMEM,
        name="gather_sum",
        compiler_params=pltpu.CompilerParams(vmem_limit_bytes=4 * 1024 * 1024),
    )(parts)


def local(
    queries,
    new_keys,
    new_values,
    cache_keys,
    cache_values,
    keep_lengths,
    cache_doc,
    new_doc,
    out_weight,
):
    ring = lax.axis_size("seq")
    packs, mesh_x, cores = lax.axis_size("dp"), lax.axis_size("x"), lax.axis_size("core")
    fresh = queries.shape[1]
    width = queries.shape[2]

    own = pack(
        keep_lengths, cache_keys[0], cache_values[0], new_keys[0], new_values[0], cache_doc, new_doc
    )
    up = [(i, (i + 1) % ring) for i in range(ring)]
    down = [(i, (i - 1) % ring) for i in range(ring)]

    hops = ring // 2
    state = None
    below = above = own
    for s in range(hops + 1):
        chunks = [below, above] if s else [own]
        if s < hops:
            if s + 1 == hops:
                below, above = below[:1], above[1:]
            below = lax.ppermute(below, "seq", up)
            above = lax.ppermute(above, "seq", down)
            if s == 0:
                other_weight = lax.ppermute(out_weight, "core", [(0, 1), (1, 0)])
            state = attend(queries[0], new_doc, chunks, state)
    (attended,) = attend(queries[0], new_doc, chunks, state, last=packs)

    each = fresh // cores
    tiles = lax.all_to_all(
        attended.reshape(packs * cores, each, width), ("dp", "core"), 0, 0, tiled=True
    ).reshape(packs, cores, each, width)
    pieces = project(tiles, out_weight, other_weight, mesh_x * cores)
    cols = pieces.shape[3]
    arrived = lax.all_to_all(
        pieces.reshape(packs * mesh_x * cores, each, cols), ("dp", "x", "core"), 0, 0, tiled=True
    )
    result = gather_sum(arrived.reshape(packs, mesh_x, cores, each, cols))
    return result.reshape(1, fresh, packs, cols)


def solution(mesh):
    shape = dict(mesh.shape)
    cores = 2
    split = Mesh(
        mesh.devices.reshape(shape["dp"], shape["seq"], shape["tensor"] // cores, cores),
        ("dp", "seq", "x", "core"),
    )
    t = ("x", "core")
    rows = P("dp", "seq", t)
    flat = P("dp", "seq")
    placed = (rows, rows, rows, rows, rows, flat, flat, flat, P(t, "dp"))

    return jax.shard_map(
        local, mesh=split, in_specs=placed, out_specs=P("dp", "seq", None, t), check_vma=False
    )
```

```python
import jax
import jax.numpy as jnp
from jax import lax
from jax.experimental import pallas as pl
from jax.experimental.pallas import tpu as pltpu
from jax.sharding import Mesh
from jax.sharding import PartitionSpec as P


HD = 128
HALVES = 2
CODES = 16
GROUPS = 4
masked_score = -1e30
to_log2 = 1.4426950408889634
VMEM = pl.BlockSpec(memory_space=pltpu.VMEM)
SMEM = pl.BlockSpec(memory_space=pltpu.SMEM)


def contract_last(a, b):
    return lax.dot_general(a, b, (((1,), (1,)), ((), ())), preferred_element_type=jnp.float32)


def dot(a, b):
    return lax.dot_general(a, b, (((1,), (0,)), ((), ())), preferred_element_type=jnp.float32)


def pack_kernel(
    keep_ref,
    queries,
    keys,
    values,
    new_keys,
    new_values,
    doc,
    new_doc,
    out_ref,
    ask_ref,
    doc_ref,
    new_doc_ref,
    sems,
):
    tokens, width = queries.shape
    slots = keys.shape[0] // HALVES
    fresh = new_keys.shape[0] // HALVES
    copies = [
        pltpu.make_async_copy(doc, doc_ref, sems.at[0]),
        pltpu.make_async_copy(new_doc, new_doc_ref, sems.at[1]),
    ]
    for h in range(HALVES):
        at = 0
        for ref, size in ((keys, slots), (values, slots), (new_keys, fresh), (new_values, fresh)):
            copies.append(
                pltpu.make_async_copy(
                    ref.at[pl.ds(h * size, size)],
                    out_ref.at[h, pl.ds(at, size)],
                    sems.at[len(copies)],
                )
            )
            at += size
    copies.append(
        pltpu.make_async_copy(queries, ask_ref.at[pl.ds(0, tokens)], sems.at[len(copies)])
    )
    for copy in copies:
        copy.start()
    copies[0].wait()
    copies[1].wait()
    lane = lax.broadcasted_iota(jnp.int32, (1, HD), 1)
    row = lax.broadcasted_iota(jnp.int32, (CODES, HD), 0)
    new_doc = new_doc_ref[...].astype(jnp.float32)
    twice = jnp.concatenate([new_doc] * (HD // new_doc.shape[1]), axis=1)
    turned = pltpu.roll(twice, fresh, 1)
    origin = lax.axis_index("seq").astype(jnp.float32)
    for h in range(HALVES):
        mine = jnp.where((lane // fresh) % HALVES == h, twice, turned)
        codes = jnp.full((CODES, HD), origin, jnp.float32)
        codes = jnp.where(row == slots // HD, mine, codes)
        for i in range(slots // HD):
            first = h * slots + i * HD
            code = doc_ref[:, pl.ds(first, HD)].astype(jnp.float32)
            code = jnp.where(lane + first < keep_ref[0, 0], code, -1.0)
            codes = jnp.where(row == i, code, codes)
        out_ref[h, pl.ds(2 * (slots + fresh), CODES), :] = codes.astype(jnp.bfloat16)
    asked = jnp.concatenate([twice, jnp.zeros((1, width - HD), jnp.float32)], axis=1)
    asked = jnp.broadcast_to(asked, (CODES, width))
    ask_ref[pl.ds(tokens, CODES), :] = asked.astype(jnp.bfloat16)
    for copy in copies[2:]:
        copy.wait()


def pack(keep, queries, keys, values, new_keys, new_values, doc, new_doc):
    rows = (keys.shape[0] + values.shape[0] + new_keys.shape[0] + new_values.shape[0]) // HALVES
    return pl.pallas_call(
        pack_kernel,
        out_shape=[
            jax.ShapeDtypeStruct((HALVES, rows + CODES, HD), jnp.bfloat16),
            jax.ShapeDtypeStruct((queries.shape[0] + CODES, queries.shape[1]), jnp.bfloat16),
        ],
        in_specs=[SMEM] + [pl.BlockSpec(memory_space=pl.ANY)] * 7,
        out_specs=[VMEM] * 2,
        scratch_shapes=[
            pltpu.VMEM(doc.shape, doc.dtype),
            pltpu.VMEM(new_doc.shape, new_doc.dtype),
            pltpu.SemaphoreType.DMA((3 + 4 * HALVES,)),
        ],
        name="pack",
        compiler_params=pltpu.CompilerParams(vmem_limit_bytes=60 * 1024 * 1024),
    )(keep, queries, keys, values, new_keys, new_values, doc, new_doc)


def attend_kernel(first, mine, last, many, *refs):
    ask_ref = refs[0]
    payloads = refs[1 : 1 + many]
    state = None if first else refs[1 + many : 4 + many]
    outs = refs[1 + many :] if first else refs[4 + many :]
    halves = [(ref, h) for ref in payloads for h in range(ref.shape[0])]
    tokens, width = ask_ref.shape
    tokens = tokens - CODES
    fresh = tokens // HALVES
    slots = (payloads[0].shape[1] - CODES - 2 * fresh) // 2
    each = slots // HD
    seq = lax.axis_index("seq")
    place = (seq if mine else seq + 1 - 2 * lax.rem(seq, 2)).astype(jnp.float32)
    lanes = lax.broadcasted_iota(jnp.int32, (1, HD), 1)
    codes = [ref[h, pl.ds(2 * (slots + fresh), CODES), :].astype(jnp.float32) for ref, h in halves]
    cache_codes = [c[i : i + 1] for c in codes for i in range(each)]
    row_fresh = jnp.full((1, HD), -1.0, jnp.float32)
    for n, c in enumerate(codes):
        seen = c[each : each + 1]
        if not (first and mine):
            seen = jnp.where(c[each + 1 : each + 2] < place, seen, -1.0)
        row_fresh = jnp.where(lanes // fresh == n, seen, row_fresh)
    new_keys = [ref[h, pl.ds(2 * slots, fresh), :] for ref, h in halves]
    new_values = [ref[h, pl.ds(2 * slots + fresh, fresh), :] for ref, h in halves]
    if len(halves) * fresh < HD:
        blank = jnp.zeros((HD - len(halves) * fresh, HD), jnp.bfloat16)
        new_keys.append(blank)
        new_values.append(blank)
    new_keys = jnp.concatenate(new_keys, axis=0)
    new_values = jnp.concatenate(new_values, axis=0)

    block = GROUPS * tokens
    square = lax.broadcasted_iota(jnp.int32, (tokens, HD), 0) == lax.broadcasted_iota(
        jnp.int32, (tokens, HD), 1
    )
    asked = ask_ref[pl.ds(tokens, CODES), pl.ds(0, HD)].astype(jnp.float32)[0:1]
    doc = jnp.sum(jnp.where(square, asked, 0.0), axis=1, keepdims=True)
    row_doc = jnp.concatenate([jnp.broadcast_to(doc, (tokens, HD))] * GROUPS, axis=0)
    scale = to_log2 * HD ** (-0.5)

    def body(b, carry):
        rows = pl.ds(pl.multiple_of(b * block, block), block)
        wide = pl.ds(pl.multiple_of(b * GROUPS * HD, GROUPS * HD), GROUPS * HD)
        q = ask_ref[pl.ds(0, tokens), wide]
        q = jnp.concatenate([q[:, g * HD : (g + 1) * HD] for g in range(GROUPS)], axis=0)
        tiles = []
        for ref, h in halves:
            scores = contract_last(q, ref[h, pl.ds(0, slots), :])
            tiles += [scores[:, i * HD : (i + 1) * HD] for i in range(each)]
        tiles = [
            jnp.where(code == row_doc, t * scale, masked_score)
            for t, code in zip(tiles, cache_codes, strict=True)
        ]
        late = contract_last(q, new_keys)
        seen = row_fresh == row_doc
        if first and mine:
            token = lax.broadcasted_iota(jnp.int32, (block, HD), 0) % tokens
            seen = seen & (lax.broadcasted_iota(jnp.int32, (block, HD), 1) <= token)
        tiles.append(jnp.where(seen, late * scale, masked_score))
        top = tiles[0]
        for t in tiles[1:]:
            top = jnp.maximum(top, t)
        top = jnp.max(top, axis=1, keepdims=True)
        if first:
            top = jnp.broadcast_to(top, (block, HD))
        else:
            before = state[1][rows, :]
            top = jnp.maximum(before, top)
            fade = jnp.exp2(before - top)
        tiles = [jnp.exp2(t - top) for t in tiles]
        total = tiles[0]
        for t in tiles[1:]:
            total = total + t
        weights = [t.astype(jnp.bfloat16) for t in tiles]
        summed = dot(weights[-1], new_values)
        for n, (ref, h) in enumerate(halves):
            part = jnp.concatenate(weights[n * each : (n + 1) * each], axis=1)
            summed = summed + dot(part, ref[h, pl.ds(slots, slots), :])
        if not first:
            total = total + state[2][rows, :] * fade
            summed = summed + state[0][rows, :] * fade
        if last:
            total = jnp.sum(total, axis=1, keepdims=True)
            outs[0][rows, :] = (summed / total).astype(jnp.bfloat16)
            level = top + jnp.log(total) * to_log2
            for i in range(block // HD):
                flat = level[i * HD : (i + 1) * HD].T
                outs[1][pl.ds(b * (block // HD) + i, 1), :] = flat[0:1]
        else:
            outs[0][rows, :] = summed
            outs[1][rows, :] = top
            outs[2][rows, :] = total
        return carry

    if last:
        outs[1][...] = jnp.zeros(outs[1].shape, jnp.float32)
    lax.fori_loop(0, width // (GROUPS * HD), body, 0)
    if last:
        level = outs[1][...]
        high = level.astype(jnp.bfloat16).astype(jnp.float32)
        middle = (level - high).astype(jnp.bfloat16).astype(jnp.float32)
        low = level - high - middle
        terms = jnp.concatenate([high, middle, low, low], axis=0).astype(jnp.bfloat16)
        outs[0][pl.ds(width // (GROUPS * HD) * block, terms.shape[0]), :] = terms


def attend(ask, payloads, state, mine, last=False):
    width = ask.shape[1]
    tokens = ask.shape[0] - CODES
    rows = tokens * width // HD
    first = state is None
    many = len(payloads)

    def kernel(*refs):
        attend_kernel(first, mine, last, many, *refs)

    scratch = []
    if last:
        out_shape = [jax.ShapeDtypeStruct((rows + 4 * 8, HD), jnp.bfloat16)]
        scratch = [pltpu.VMEM((8, HD), jnp.float32)]
    else:
        out_shape = [jax.ShapeDtypeStruct((rows, HD), jnp.float32)] * 3
    args = (ask, *payloads, *(() if first else state))
    keys = sum(p.shape[0] * p.shape[1] for p in payloads) // 2
    return pl.pallas_call(
        kernel,
        out_shape=out_shape,
        in_specs=[VMEM] * len(args),
        out_specs=[VMEM] * len(out_shape),
        scratch_shapes=scratch,
        name="attend_last" if last else ("attend_first" if first else "attend_step"),
        cost_estimate=pl.CostEstimate(
            flops=16 * rows * keys * HD,
            bytes_accessed=keys * HD * 4 + 6 * rows * HD * 4,
            transcendentals=rows * keys,
        ),
        compiler_params=pltpu.CompilerParams(vmem_limit_bytes=12 * 1024 * 1024),
    )(*args)


def merge_kernel(summed_ref, top_ref, total_ref, other_ref, out_ref):
    copies, tokens, _ = out_ref.shape
    rows = summed_ref.shape[0]
    terms = other_ref[pl.ds(rows, 4 * 8), :].astype(jnp.float32)
    level = terms[0:8] + terms[8:16] + terms[16:24]
    for i in range(rows // HD):
        at = pl.ds(i * HD, HD)
        other = jnp.broadcast_to(level[i : i + 1], (HD, HD)).T
        top = jnp.maximum(top_ref[at, :], other)
        mine = jnp.exp2(top_ref[at, :] - top)
        theirs = jnp.exp2(other - top)
        total = jnp.sum(total_ref[at, :], axis=1, keepdims=True) * mine + theirs
        summed = summed_ref[at, :] * mine + other_ref[at, :].astype(jnp.float32) * theirs
        value = (summed / total).astype(jnp.bfloat16)
        for g in range(HD // tokens):
            head = i * (HD // tokens) + g
            for copy in range(copies):
                out_ref[copy, :, pl.ds(head * HD, HD)] = value[g * tokens : (g + 1) * tokens]


def merge(state, other, copies, tokens):
    rows = state[0].shape[0]
    return pl.pallas_call(
        merge_kernel,
        out_shape=jax.ShapeDtypeStruct((copies, tokens, rows // tokens * HD), jnp.bfloat16),
        in_specs=[VMEM] * 4,
        out_specs=VMEM,
        name="merge",
        compiler_params=pltpu.CompilerParams(vmem_limit_bytes=8 * 1024 * 1024),
    )(*state, other)


def project_kernel(a_ref, own_ref, other_ref, out_ref):
    core = lax.axis_index("core")
    packs, each, width = a_ref.shape[0], a_ref.shape[2], a_ref.shape[3]
    pieces, cols = out_ref.shape[1], out_ref.shape[3]
    mine = a_ref[:, core].reshape(packs * each, width)
    theirs = a_ref[:, 1 - core].reshape(packs * each, width)
    for j in range(pieces):
        at = pl.ds(j * cols, cols)
        summed = dot(mine, own_ref[:, at]) + dot(theirs, other_ref[:, at])
        out_ref[:, j] = summed.astype(jnp.bfloat16).reshape(packs, each, cols)


def project(a, own, other, pieces):
    packs, _, each, width = a.shape
    cols = own.shape[1] // pieces
    block = 2
    return pl.pallas_call(
        project_kernel,
        grid=(pieces // block,),
        out_shape=jax.ShapeDtypeStruct((packs, pieces, each, cols), jnp.bfloat16),
        in_specs=[
            pl.BlockSpec(a.shape, lambda j: (0, 0, 0, 0)),
            pl.BlockSpec((width, cols * block), lambda j: (0, j)),
            pl.BlockSpec((width, cols * block), lambda j: (0, j)),
        ],
        out_specs=pl.BlockSpec((packs, block, each, cols), lambda j: (0, j, 0, 0)),
        name="project",
        cost_estimate=pl.CostEstimate(
            flops=4 * packs * each * width * own.shape[1],
            bytes_accessed=4 * width * own.shape[1],
            transcendentals=0,
        ),
        compiler_params=pltpu.CompilerParams(vmem_limit_bytes=16 * 1024 * 1024),
    )(a, own, other)


def gather_sum_kernel(parts_ref, out_ref):
    packs, terms, cores, each, cols = parts_ref.shape
    for d in range(packs):
        for c in range(cores):
            total = parts_ref[d, 0, c].astype(jnp.float32)
            for t in range(1, terms):
                total = total + parts_ref[d, t, c].astype(jnp.float32)
            out_ref[pl.ds(c * each, each), pl.ds(d * cols, cols)] = total.astype(jnp.bfloat16)


def gather_sum(parts):
    packs, _, cores, each, cols = parts.shape
    return pl.pallas_call(
        gather_sum_kernel,
        out_shape=jax.ShapeDtypeStruct((cores * each, packs * cols), jnp.bfloat16),
        in_specs=[VMEM],
        out_specs=VMEM,
        name="gather_sum",
        compiler_params=pltpu.CompilerParams(vmem_limit_bytes=4 * 1024 * 1024),
    )(parts)


def local(
    queries,
    new_keys,
    new_values,
    cache_keys,
    cache_values,
    keep_lengths,
    cache_doc,
    new_doc,
    out_weight,
):
    ring = lax.axis_size("seq")
    packs, mesh_x, cores = lax.axis_size("dp"), lax.axis_size("x"), lax.axis_size("core")
    fresh = queries.shape[1]
    width = queries.shape[2]

    own, ask = pack(
        keep_lengths,
        queries[0],
        cache_keys[0],
        cache_values[0],
        new_keys[0],
        new_values[0],
        cache_doc,
        new_doc,
    )
    up = [(i, (i + 2) % ring) for i in range(ring)]
    down = [(i, (i - 2) % ring) for i in range(ring)]
    pair = [(i, i + 1 - 2 * (i % 2)) for i in range(ring)]
    hops = ring // 4
    state = other = None
    below = above = own
    for s in range(hops + 1):
        chunks = [below, above] if s else [own]
        if s < hops:
            if s + 1 == hops:
                below, above = below[:1], above[1:]
            below = lax.ppermute(below, "seq", up)
            above = lax.ppermute(above, "seq", down)
            if s == 0:
                asked = lax.ppermute(ask, "seq", pair)
                other_weight = lax.ppermute(out_weight, "core", [(0, 1), (1, 0)])
            state = attend(ask, chunks, state, True)
            other = attend(asked, chunks, other, False)
    (other,) = attend(asked, chunks, other, False, last=True)
    other = lax.ppermute(other, "seq", pair)
    state = attend(ask, chunks, state, True)
    attended = merge(state, other, packs, fresh)

    each = fresh // cores
    tiles = lax.all_to_all(
        attended.reshape(packs * cores, each, width), ("dp", "core"), 0, 0, tiled=True
    ).reshape(packs, cores, each, width)
    pieces = project(tiles, out_weight, other_weight, mesh_x * cores)
    cols = pieces.shape[3]
    arrived = lax.all_to_all(
        pieces.reshape(packs * mesh_x * cores, each, cols), ("dp", "x", "core"), 0, 0, tiled=True
    )
    result = gather_sum(arrived.reshape(packs, mesh_x, cores, each, cols))
    return result.reshape(1, fresh, packs, cols)


def solution(mesh):
    shape = dict(mesh.shape)
    cores = 2
    split = Mesh(
        mesh.devices.reshape(shape["dp"], shape["seq"], shape["tensor"] // cores, cores),
        ("dp", "seq", "x", "core"),
    )
    t = ("x", "core")
    rows = P("dp", "seq", t)
    flat = P("dp", "seq")
    placed = (rows, rows, rows, rows, rows, flat, flat, flat, P(t, "dp"))

    return jax.shard_map(
        local, mesh=split, in_specs=placed, out_specs=P("dp", "seq", None, t), check_vma=False
    )
```

```python
import jax
import jax.numpy as jnp
from jax import lax
from jax.experimental import pallas as pl
from jax.experimental.pallas import tpu as pltpu
from jax.sharding import Mesh
from jax.sharding import PartitionSpec as P


HD = 128
HALVES = 2
CODES = 16
GROUPS = 4
masked_score = -1e30
to_log2 = 1.4426950408889634
VMEM = pl.BlockSpec(memory_space=pltpu.VMEM)
SMEM = pl.BlockSpec(memory_space=pltpu.SMEM)


def contract_last(a, b):
    return lax.dot_general(a, b, (((1,), (1,)), ((), ())), preferred_element_type=jnp.float32)


def dot(a, b):
    return lax.dot_general(a, b, (((1,), (0,)), ((), ())), preferred_element_type=jnp.float32)


def pack_kernel(
    keep_ref,
    queries,
    keys,
    values,
    new_keys,
    new_values,
    doc,
    new_doc,
    out_ref,
    ask_ref,
    doc_ref,
    new_doc_ref,
    sems,
):
    tokens, width = queries.shape
    slots = keys.shape[0] // HALVES
    fresh = new_keys.shape[0] // HALVES
    copies = [
        pltpu.make_async_copy(doc, doc_ref, sems.at[0]),
        pltpu.make_async_copy(new_doc, new_doc_ref, sems.at[1]),
    ]
    for h in range(HALVES):
        at = 0
        for ref, size in ((keys, slots), (values, slots), (new_keys, fresh), (new_values, fresh)):
            copies.append(
                pltpu.make_async_copy(
                    ref.at[pl.ds(h * size, size)],
                    out_ref.at[h, pl.ds(at, size)],
                    sems.at[len(copies)],
                )
            )
            at += size
    copies.append(
        pltpu.make_async_copy(queries, ask_ref.at[pl.ds(0, tokens)], sems.at[len(copies)])
    )
    for copy in copies:
        copy.start()
    copies[0].wait()
    copies[1].wait()
    lane = lax.broadcasted_iota(jnp.int32, (1, HD), 1)
    row = lax.broadcasted_iota(jnp.int32, (CODES, HD), 0)
    new_doc = new_doc_ref[...].astype(jnp.float32)
    twice = jnp.concatenate([new_doc] * (HD // new_doc.shape[1]), axis=1)
    turned = pltpu.roll(twice, fresh, 1)
    origin = lax.axis_index("seq").astype(jnp.float32)
    for h in range(HALVES):
        mine = jnp.where((lane // fresh) % HALVES == h, twice, turned)
        codes = jnp.full((CODES, HD), origin, jnp.float32)
        codes = jnp.where(row == slots // HD, mine, codes)
        for i in range(slots // HD):
            first = h * slots + i * HD
            code = doc_ref[:, pl.ds(first, HD)].astype(jnp.float32)
            code = jnp.where(lane + first < keep_ref[0, 0], code, -1.0)
            codes = jnp.where(row == i, code, codes)
        out_ref[h, pl.ds(2 * (slots + fresh), CODES), :] = codes.astype(jnp.bfloat16)
    asked = jnp.concatenate([twice, jnp.zeros((1, width - HD), jnp.float32)], axis=1)
    asked = jnp.broadcast_to(asked, (CODES, width))
    ask_ref[pl.ds(tokens, CODES), :] = asked.astype(jnp.bfloat16)
    for copy in copies[2:]:
        copy.wait()


def pack(keep, queries, keys, values, new_keys, new_values, doc, new_doc):
    rows = (keys.shape[0] + values.shape[0] + new_keys.shape[0] + new_values.shape[0]) // HALVES
    return pl.pallas_call(
        pack_kernel,
        out_shape=[
            jax.ShapeDtypeStruct((HALVES, rows + CODES, HD), jnp.bfloat16),
            jax.ShapeDtypeStruct((queries.shape[0] + CODES, queries.shape[1]), jnp.bfloat16),
        ],
        in_specs=[SMEM] + [pl.BlockSpec(memory_space=pl.ANY)] * 7,
        out_specs=[VMEM] * 2,
        scratch_shapes=[
            pltpu.VMEM(doc.shape, doc.dtype),
            pltpu.VMEM(new_doc.shape, new_doc.dtype),
            pltpu.SemaphoreType.DMA((3 + 4 * HALVES,)),
        ],
        name="pack",
        compiler_params=pltpu.CompilerParams(vmem_limit_bytes=60 * 1024 * 1024),
    )(keep, queries, keys, values, new_keys, new_values, doc, new_doc)


def attend_kernel(first, mine, last, many, *refs):
    ask_ref = refs[0]
    payloads = refs[1 : 1 + many]
    state = None if first else refs[1 + many : 4 + many]
    outs = refs[1 + many :] if first else refs[4 + many :]
    halves = [(ref, h) for ref in payloads for h in range(ref.shape[0])]
    tokens, width = ask_ref.shape
    tokens = tokens - CODES
    fresh = tokens // HALVES
    slots = (payloads[0].shape[1] - CODES - 2 * fresh) // 2
    each = slots // HD
    seq = lax.axis_index("seq")
    place = (seq if mine else seq + 1 - 2 * lax.rem(seq, 2)).astype(jnp.float32)
    lanes = lax.broadcasted_iota(jnp.int32, (1, HD), 1)
    codes = [ref[h, pl.ds(2 * (slots + fresh), CODES), :].astype(jnp.float32) for ref, h in halves]
    cache_codes = [c[i : i + 1] for c in codes for i in range(each)]
    row_fresh = jnp.full((1, HD), -1.0, jnp.float32)
    for n, c in enumerate(codes):
        seen = c[each : each + 1]
        if not (first and mine):
            seen = jnp.where(c[each + 1 : each + 2] < place, seen, -1.0)
        row_fresh = jnp.where(lanes // fresh == n, seen, row_fresh)
    new_keys = [ref[h, pl.ds(2 * slots, fresh), :] for ref, h in halves]
    new_values = [ref[h, pl.ds(2 * slots + fresh, fresh), :] for ref, h in halves]
    if len(halves) * fresh < HD:
        blank = jnp.zeros((HD - len(halves) * fresh, HD), jnp.bfloat16)
        new_keys.append(blank)
        new_values.append(blank)
    new_keys = jnp.concatenate(new_keys, axis=0)
    new_values = jnp.concatenate(new_values, axis=0)

    block = GROUPS * tokens
    square = lax.broadcasted_iota(jnp.int32, (tokens, HD), 0) == lax.broadcasted_iota(
        jnp.int32, (tokens, HD), 1
    )
    asked = ask_ref[pl.ds(tokens, CODES), pl.ds(0, HD)].astype(jnp.float32)[0:1]
    doc = jnp.sum(jnp.where(square, asked, 0.0), axis=1, keepdims=True)
    row_doc = jnp.concatenate([jnp.broadcast_to(doc, (tokens, HD))] * GROUPS, axis=0)
    scale = to_log2 * HD ** (-0.5)

    def body(b, carry):
        rows = pl.ds(pl.multiple_of(b * block, block), block)
        wide = pl.ds(pl.multiple_of(b * GROUPS * HD, GROUPS * HD), GROUPS * HD)
        q = ask_ref[pl.ds(0, tokens), wide]
        q = jnp.concatenate([q[:, g * HD : (g + 1) * HD] for g in range(GROUPS)], axis=0)
        tiles = []
        for ref, h in halves:
            scores = contract_last(q, ref[h, pl.ds(0, slots), :])
            tiles += [scores[:, i * HD : (i + 1) * HD] for i in range(each)]
        tiles = [
            jnp.where(code == row_doc, t * scale, masked_score)
            for t, code in zip(tiles, cache_codes, strict=True)
        ]
        late = contract_last(q, new_keys)
        seen = row_fresh == row_doc
        if first and mine:
            token = lax.broadcasted_iota(jnp.int32, (block, HD), 0) % tokens
            seen = seen & (lax.broadcasted_iota(jnp.int32, (block, HD), 1) <= token)
        tiles.append(jnp.where(seen, late * scale, masked_score))
        top = tiles[0]
        for t in tiles[1:]:
            top = jnp.maximum(top, t)
        top = jnp.max(top, axis=1, keepdims=True)
        if first:
            top = jnp.broadcast_to(top, (block, HD))
        else:
            before = state[1][rows, :]
            top = jnp.maximum(before, top)
            fade = jnp.exp2(before - top)
        tiles = [jnp.exp2(t - top) for t in tiles]
        total = tiles[0]
        for t in tiles[1:]:
            total = total + t
        weights = [t.astype(jnp.bfloat16) for t in tiles]
        summed = dot(weights[-1], new_values)
        for n, (ref, h) in enumerate(halves):
            part = jnp.concatenate(weights[n * each : (n + 1) * each], axis=1)
            summed = summed + dot(part, ref[h, pl.ds(slots, slots), :])
        if not first:
            total = total + state[2][rows, :] * fade
            summed = summed + state[0][rows, :] * fade
        if last:
            total = jnp.sum(total, axis=1, keepdims=True)
            outs[0][rows, :] = (summed / total).astype(jnp.bfloat16)
            level = top + jnp.log(total) * to_log2
            for i in range(block // HD):
                flat = level[i * HD : (i + 1) * HD].T
                outs[1][pl.ds(b * (block // HD) + i, 1), :] = flat[0:1]
        else:
            outs[0][rows, :] = summed
            outs[1][rows, :] = top
            outs[2][rows, :] = total
        return carry

    if last:
        outs[1][...] = jnp.zeros(outs[1].shape, jnp.float32)
    lax.fori_loop(0, width // (GROUPS * HD), body, 0)
    if last:
        level = outs[1][...]
        high = level.astype(jnp.bfloat16).astype(jnp.float32)
        middle = (level - high).astype(jnp.bfloat16).astype(jnp.float32)
        low = level - high - middle
        terms = jnp.concatenate([high, middle, low, low], axis=0).astype(jnp.bfloat16)
        outs[0][pl.ds(width // (GROUPS * HD) * block, terms.shape[0]), :] = terms


def attend(ask, payloads, state, mine, last=False):
    width = ask.shape[1]
    tokens = ask.shape[0] - CODES
    rows = tokens * width // HD
    first = state is None
    many = len(payloads)

    def kernel(*refs):
        attend_kernel(first, mine, last, many, *refs)

    scratch = []
    if last:
        out_shape = [jax.ShapeDtypeStruct((rows + 4 * 8, HD), jnp.bfloat16)]
        scratch = [pltpu.VMEM((8, HD), jnp.float32)]
    else:
        out_shape = [jax.ShapeDtypeStruct((rows, HD), jnp.float32)] * 3
    args = (ask, *payloads, *(() if first else state))
    keys = sum(p.shape[0] * p.shape[1] for p in payloads) // 2
    return pl.pallas_call(
        kernel,
        out_shape=out_shape,
        in_specs=[VMEM] * len(args),
        out_specs=[VMEM] * len(out_shape),
        scratch_shapes=scratch,
        name="attend_last" if last else ("attend_first" if first else "attend_step"),
        cost_estimate=pl.CostEstimate(
            flops=16 * rows * keys * HD,
            bytes_accessed=keys * HD * 4 + 6 * rows * HD * 4,
            transcendentals=rows * keys,
        ),
        compiler_params=pltpu.CompilerParams(vmem_limit_bytes=12 * 1024 * 1024),
    )(*args)


def merge_kernel(summed_ref, top_ref, total_ref, other_ref, out_ref):
    copies, tokens, _ = out_ref.shape
    rows = summed_ref.shape[0]
    terms = other_ref[pl.ds(rows, 4 * 8), :].astype(jnp.float32)
    level = terms[0:8] + terms[8:16] + terms[16:24]
    for i in range(rows // HD):
        at = pl.ds(i * HD, HD)
        other = jnp.broadcast_to(level[i : i + 1], (HD, HD)).T
        top = jnp.maximum(top_ref[at, :], other)
        mine = jnp.exp2(top_ref[at, :] - top)
        theirs = jnp.exp2(other - top)
        total = jnp.sum(total_ref[at, :], axis=1, keepdims=True) * mine + theirs
        summed = summed_ref[at, :] * mine + other_ref[at, :].astype(jnp.float32) * theirs
        value = (summed / total).astype(jnp.bfloat16)
        for g in range(HD // tokens):
            head = i * (HD // tokens) + g
            for copy in range(copies):
                out_ref[copy, :, pl.ds(head * HD, HD)] = value[g * tokens : (g + 1) * tokens]


def merge(state, other, copies, tokens):
    rows = state[0].shape[0]
    return pl.pallas_call(
        merge_kernel,
        out_shape=jax.ShapeDtypeStruct((copies, tokens, rows // tokens * HD), jnp.bfloat16),
        in_specs=[VMEM] * 4,
        out_specs=VMEM,
        name="merge",
        compiler_params=pltpu.CompilerParams(vmem_limit_bytes=8 * 1024 * 1024),
    )(*state, other)


def project_kernel(a_ref, own_ref, other_ref, out_ref):
    core = lax.axis_index("core")
    packs, each, width = a_ref.shape[0], a_ref.shape[2], a_ref.shape[3]
    pieces, cols = out_ref.shape[1], out_ref.shape[3]
    mine = a_ref[:, core].reshape(packs * each, width)
    theirs = a_ref[:, 1 - core].reshape(packs * each, width)
    for j in range(pieces):
        at = pl.ds(j * cols, cols)
        summed = dot(mine, own_ref[:, at]) + dot(theirs, other_ref[:, at])
        out_ref[:, j] = summed.astype(jnp.bfloat16).reshape(packs, each, cols)


def project(a, own, other, pieces):
    packs, _, each, width = a.shape
    cols = own.shape[1] // pieces
    block = 2
    return pl.pallas_call(
        project_kernel,
        grid=(pieces // block,),
        out_shape=jax.ShapeDtypeStruct((packs, pieces, each, cols), jnp.bfloat16),
        in_specs=[
            pl.BlockSpec(a.shape, lambda j: (0, 0, 0, 0)),
            pl.BlockSpec((width, cols * block), lambda j: (0, j)),
            pl.BlockSpec((width, cols * block), lambda j: (0, j)),
        ],
        out_specs=pl.BlockSpec((packs, block, each, cols), lambda j: (0, j, 0, 0)),
        name="project",
        cost_estimate=pl.CostEstimate(
            flops=4 * packs * each * width * own.shape[1],
            bytes_accessed=4 * width * own.shape[1],
            transcendentals=0,
        ),
        compiler_params=pltpu.CompilerParams(vmem_limit_bytes=16 * 1024 * 1024),
    )(a, own, other)


def gather_sum_kernel(parts_ref, out_ref):
    packs, terms, cores, each, _ = parts_ref.shape
    for c in range(cores):
        blocks = []
        for d in range(packs):
            total = parts_ref[d, 0, c].astype(jnp.float32)
            for t in range(1, terms):
                total = total + parts_ref[d, t, c].astype(jnp.float32)
            blocks.append(total)
        out_ref[pl.ds(c * each, each)] = jnp.stack(blocks, axis=1).astype(jnp.bfloat16)


def gather_sum(parts):
    packs, _, cores, each, cols = parts.shape
    return pl.pallas_call(
        gather_sum_kernel,
        out_shape=jax.ShapeDtypeStruct((cores * each, packs, cols), jnp.bfloat16),
        in_specs=[VMEM],
        out_specs=VMEM,
        name="gather_sum",
        compiler_params=pltpu.CompilerParams(vmem_limit_bytes=4 * 1024 * 1024),
    )(parts)


def local(
    queries,
    new_keys,
    new_values,
    cache_keys,
    cache_values,
    keep_lengths,
    cache_doc,
    new_doc,
    out_weight,
):
    ring = lax.axis_size("seq")
    packs, mesh_x, cores = lax.axis_size("dp"), lax.axis_size("x"), lax.axis_size("core")
    fresh = queries.shape[1]
    width = queries.shape[2]

    own, ask = pack(
        keep_lengths,
        queries[0],
        cache_keys[0],
        cache_values[0],
        new_keys[0],
        new_values[0],
        cache_doc,
        new_doc,
    )
    up = [(i, (i + 2) % ring) for i in range(ring)]
    down = [(i, (i - 2) % ring) for i in range(ring)]
    pair = [(i, i + 1 - 2 * (i % 2)) for i in range(ring)]
    hops = ring // 4
    state = other = None
    below = above = own
    for s in range(hops + 1):
        chunks = [below, above] if s else [own]
        if s < hops:
            if s + 1 == hops:
                below, above = below[:1], above[1:]
            below = lax.ppermute(below, "seq", up)
            above = lax.ppermute(above, "seq", down)
            if s == 0:
                asked = lax.ppermute(ask, "seq", pair)
                other_weight = lax.ppermute(out_weight, "core", [(0, 1), (1, 0)])
            state = attend(ask, chunks, state, True)
            other = attend(asked, chunks, other, False)
    (other,) = attend(asked, chunks, other, False, last=True)
    other = lax.ppermute(other, "seq", pair)
    state = attend(ask, chunks, state, True)
    attended = merge(state, other, packs, fresh)

    each = fresh // cores
    tiles = lax.all_to_all(
        attended.reshape(packs * cores, each, width), ("dp", "core"), 0, 0, tiled=True
    ).reshape(packs, cores, each, width)
    pieces = project(tiles, out_weight, other_weight, mesh_x * cores)
    cols = pieces.shape[3]
    arrived = lax.all_to_all(
        pieces.reshape(packs * mesh_x * cores, each, cols), ("dp", "x", "core"), 0, 0, tiled=True
    )
    result = gather_sum(arrived.reshape(packs, mesh_x, cores, each, cols))
    return result[None]


def solution(mesh):
    shape = dict(mesh.shape)
    cores = 2
    split = Mesh(
        mesh.devices.reshape(shape["dp"], shape["seq"], shape["tensor"] // cores, cores),
        ("dp", "seq", "x", "core"),
    )
    t = ("x", "core")
    rows = P("dp", "seq", t)
    flat = P("dp", "seq")
    placed = (rows, rows, rows, rows, rows, flat, flat, flat, P(t, "dp"))

    return jax.shard_map(
        local, mesh=split, in_specs=placed, out_specs=P("dp", "seq", None, t), check_vma=False
    )
```

```python
import jax
import jax.numpy as jnp
from jax import lax
from jax.experimental import pallas as pl
from jax.experimental.pallas import tpu as pltpu
from jax.sharding import Mesh
from jax.sharding import PartitionSpec as P


HD = 128
HALVES = 2
CODES = 8
GROUPS = 4
CORES = 2
masked_score = -1e30
to_log2 = 1.4426950408889634
VMEM = pl.BlockSpec(memory_space=pltpu.VMEM)
SMEM = pl.BlockSpec(memory_space=pltpu.SMEM)


def contract_last(a, b):
    return lax.dot_general(a, b, (((1,), (1,)), ((), ())), preferred_element_type=jnp.float32)


def dot(a, b):
    return lax.dot_general(a, b, (((1,), (0,)), ((), ())), preferred_element_type=jnp.float32)


def pack_kernel(
    keep_ref,
    queries,
    keys,
    values,
    new_keys,
    new_values,
    doc,
    new_doc,
    out_ref,
    ask_ref,
    doc_ref,
    new_doc_ref,
    sems,
):
    tokens, width = queries.shape
    slots = keys.shape[0] // HALVES
    fresh = new_keys.shape[0] // HALVES
    copies = [
        pltpu.make_async_copy(doc, doc_ref, sems.at[0]),
        pltpu.make_async_copy(new_doc, new_doc_ref, sems.at[1]),
    ]
    for h in range(HALVES):
        at = 0
        for ref, size in ((keys, slots), (values, slots), (new_keys, fresh), (new_values, fresh)):
            copies.append(
                pltpu.make_async_copy(
                    ref.at[pl.ds(h * size, size)],
                    out_ref.at[h, pl.ds(at, size)],
                    sems.at[len(copies)],
                )
            )
            at += size
    copies.append(
        pltpu.make_async_copy(queries, ask_ref.at[pl.ds(0, tokens)], sems.at[len(copies)])
    )
    for copy in copies:
        copy.start()
    copies[0].wait()
    copies[1].wait()
    lane = lax.broadcasted_iota(jnp.int32, (1, HD), 1)
    row = lax.broadcasted_iota(jnp.int32, (CODES, HD), 0)
    new_doc = new_doc_ref[...].astype(jnp.float32)
    twice = jnp.concatenate([new_doc] * (HD // new_doc.shape[1]), axis=1)
    turned = pltpu.roll(twice, fresh, 1)
    origin = lax.axis_index("seq").astype(jnp.float32)
    for h in range(HALVES):
        mine = jnp.where((lane // fresh) % HALVES == h, twice, turned)
        codes = jnp.full((CODES, HD), origin, jnp.float32)
        codes = jnp.where(row == slots // HD, mine, codes)
        for i in range(slots // HD):
            first = h * slots + i * HD
            code = doc_ref[:, pl.ds(first, HD)].astype(jnp.float32)
            code = jnp.where(lane + first < keep_ref[0, 0], code, -1.0)
            codes = jnp.where(row == i, code, codes)
        out_ref[h, pl.ds(2 * (slots + fresh), CODES), :] = codes.astype(jnp.bfloat16)
    asked = jnp.concatenate([twice, jnp.zeros((1, width - HD), jnp.float32)], axis=1)
    asked = jnp.broadcast_to(asked, (CODES, width))
    ask_ref[pl.ds(tokens, CODES), :] = asked.astype(jnp.bfloat16)
    for copy in copies[2:]:
        copy.wait()


def pack(keep, queries, keys, values, new_keys, new_values, doc, new_doc):
    rows = (keys.shape[0] + values.shape[0] + new_keys.shape[0] + new_values.shape[0]) // HALVES
    return pl.pallas_call(
        pack_kernel,
        out_shape=[
            jax.ShapeDtypeStruct((HALVES, rows + CODES, HD), jnp.bfloat16),
            jax.ShapeDtypeStruct((queries.shape[0] + CODES, queries.shape[1]), jnp.bfloat16),
        ],
        in_specs=[SMEM] + [pl.BlockSpec(memory_space=pl.ANY)] * 7,
        out_specs=[VMEM] * 2,
        scratch_shapes=[
            pltpu.VMEM(doc.shape, doc.dtype),
            pltpu.VMEM(new_doc.shape, new_doc.dtype),
            pltpu.SemaphoreType.DMA((3 + 4 * HALVES,)),
        ],
        name="pack",
        compiler_params=pltpu.CompilerParams(vmem_limit_bytes=60 * 1024 * 1024),
    )(keep, queries, keys, values, new_keys, new_values, doc, new_doc)


def attend_kernel(first, mine, last, many, *refs):
    ask_ref = refs[0]
    payloads = refs[1 : 1 + many]
    state = None if first else refs[1 + many : 4 + many]
    outs = refs[1 + many :] if first else refs[4 + many :]
    halves = [(ref, h) for ref in payloads for h in range(ref.shape[0])]
    tokens, width = ask_ref.shape
    tokens = tokens - CODES
    fresh = tokens // HALVES
    slots = (payloads[0].shape[1] - CODES - 2 * fresh) // 2
    each = slots // HD
    seq = lax.axis_index("seq")
    place = (seq if mine else seq + 1 - 2 * lax.rem(seq, 2)).astype(jnp.float32)
    lanes = lax.broadcasted_iota(jnp.int32, (1, HD), 1)
    codes = [ref[h, pl.ds(2 * (slots + fresh), CODES), :].astype(jnp.float32) for ref, h in halves]
    cache_codes = [c[i : i + 1] for c in codes for i in range(each)]
    row_fresh = jnp.full((1, HD), -1.0, jnp.float32)
    for n, c in enumerate(codes):
        seen = c[each : each + 1]
        if not (first and mine):
            seen = jnp.where(c[each + 1 : each + 2] < place, seen, -1.0)
        row_fresh = jnp.where(lanes // fresh == n, seen, row_fresh)
    new_keys = [ref[h, pl.ds(2 * slots, fresh), :] for ref, h in halves]
    new_values = [ref[h, pl.ds(2 * slots + fresh, fresh), :] for ref, h in halves]
    if len(halves) * fresh < HD:
        blank = jnp.zeros((HD - len(halves) * fresh, HD), jnp.bfloat16)
        new_keys.append(blank)
        new_values.append(blank)
    new_keys = jnp.concatenate(new_keys, axis=0)
    new_values = jnp.concatenate(new_values, axis=0)

    block = GROUPS * tokens
    square = lax.broadcasted_iota(jnp.int32, (tokens, HD), 0) == lax.broadcasted_iota(
        jnp.int32, (tokens, HD), 1
    )
    asked = ask_ref[pl.ds(tokens, CODES), pl.ds(0, HD)].astype(jnp.float32)[0:1]
    doc = jnp.sum(jnp.where(square, asked, 0.0), axis=1, keepdims=True)
    row_doc = jnp.concatenate([jnp.broadcast_to(doc, (tokens, HD))] * GROUPS, axis=0)
    scale = to_log2 * HD ** (-0.5)

    def body(b, carry):
        rows = pl.ds(pl.multiple_of(b * block, block), block)
        wide = pl.ds(pl.multiple_of(b * GROUPS * HD, GROUPS * HD), GROUPS * HD)
        q = ask_ref[pl.ds(0, tokens), wide]
        q = jnp.concatenate([q[:, g * HD : (g + 1) * HD] for g in range(GROUPS)], axis=0)
        tiles = []
        for ref, h in halves:
            scores = contract_last(q, ref[h, pl.ds(0, slots), :])
            tiles += [scores[:, i * HD : (i + 1) * HD] for i in range(each)]
        tiles = [
            jnp.where(code == row_doc, t * scale, masked_score)
            for t, code in zip(tiles, cache_codes, strict=True)
        ]
        late = contract_last(q, new_keys)
        seen = row_fresh == row_doc
        if first and mine:
            token = lax.broadcasted_iota(jnp.int32, (block, HD), 0) % tokens
            seen = seen & (lax.broadcasted_iota(jnp.int32, (block, HD), 1) <= token)
        tiles.append(jnp.where(seen, late * scale, masked_score))
        top = tiles[0]
        for t in tiles[1:]:
            top = jnp.maximum(top, t)
        top = jnp.max(top, axis=1, keepdims=True)
        if first:
            top = jnp.broadcast_to(top, (block, HD))
        else:
            before = state[1][rows, :]
            top = jnp.maximum(before, top)
            fade = jnp.exp2(before - top)
        tiles = [jnp.exp2(t - top) for t in tiles]
        total = tiles[0]
        for t in tiles[1:]:
            total = total + t
        weights = [t.astype(jnp.bfloat16) for t in tiles]
        summed = dot(weights[-1], new_values)
        for n, (ref, h) in enumerate(halves):
            part = jnp.concatenate(weights[n * each : (n + 1) * each], axis=1)
            summed = summed + dot(part, ref[h, pl.ds(slots, slots), :])
        if not first:
            total = total + state[2][rows, :] * fade
            summed = summed + state[0][rows, :] * fade
        if last:
            total = jnp.sum(total, axis=1, keepdims=True)
            outs[0][rows, :] = (summed / total).astype(jnp.bfloat16)
            level = top + jnp.log(total) * to_log2
            for i in range(block // HD):
                flat = level[i * HD : (i + 1) * HD].T
                outs[1][pl.ds(b * (block // HD) + i, 1), :] = flat[0:1]
        else:
            outs[0][rows, :] = summed
            outs[1][rows, :] = top
            outs[2][rows, :] = total
        return carry

    if last:
        outs[1][...] = jnp.zeros(outs[1].shape, jnp.float32)
    lax.fori_loop(0, width // (GROUPS * HD), body, 0)
    if last:
        level = outs[1][...]
        high = level.astype(jnp.bfloat16).astype(jnp.float32)
        middle = (level - high).astype(jnp.bfloat16).astype(jnp.float32)
        low = level - high - middle
        terms = jnp.concatenate([high, middle, low, low], axis=0).astype(jnp.bfloat16)
        outs[0][pl.ds(width // (GROUPS * HD) * block, terms.shape[0]), :] = terms


def attend(ask, payloads, state, mine, last=False):
    width = ask.shape[1]
    tokens = ask.shape[0] - CODES
    rows = tokens * width // HD
    first = state is None
    many = len(payloads)

    def kernel(*refs):
        attend_kernel(first, mine, last, many, *refs)

    scratch = []
    if last:
        out_shape = [jax.ShapeDtypeStruct((rows + 4 * 8, HD), jnp.bfloat16)]
        scratch = [pltpu.VMEM((8, HD), jnp.float32)]
    else:
        out_shape = [jax.ShapeDtypeStruct((rows, HD), jnp.float32)] * 3
    args = (ask, *payloads, *(() if first else state))
    keys = sum(p.shape[0] * p.shape[1] for p in payloads) // 2
    return pl.pallas_call(
        kernel,
        out_shape=out_shape,
        in_specs=[VMEM] * len(args),
        out_specs=[VMEM] * len(out_shape),
        scratch_shapes=scratch,
        name="attend_last" if last else ("attend_first" if first else "attend_step"),
        cost_estimate=pl.CostEstimate(
            flops=16 * rows * keys * HD,
            bytes_accessed=keys * HD * 4 + 6 * rows * HD * 4,
            transcendentals=rows * keys,
        ),
        compiler_params=pltpu.CompilerParams(vmem_limit_bytes=12 * 1024 * 1024),
    )(*args)


def merge_kernel(summed_ref, top_ref, total_ref, other_ref, out_ref):
    copies, tokens, _ = out_ref.shape
    rows = summed_ref.shape[0]
    terms = other_ref[pl.ds(rows, 4 * 8), :].astype(jnp.float32)
    level = terms[0:8] + terms[8:16] + terms[16:24]
    for i in range(rows // HD):
        at = pl.ds(i * HD, HD)
        other = jnp.broadcast_to(level[i : i + 1], (HD, HD)).T
        top = jnp.maximum(top_ref[at, :], other)
        mine = jnp.exp2(top_ref[at, :] - top)
        theirs = jnp.exp2(other - top)
        total = jnp.sum(total_ref[at, :], axis=1, keepdims=True) * mine + theirs
        summed = summed_ref[at, :] * mine + other_ref[at, :].astype(jnp.float32) * theirs
        value = (summed / total).astype(jnp.bfloat16)
        for g in range(HD // tokens):
            head = i * (HD // tokens) + g
            for copy in range(copies):
                out_ref[copy, :, pl.ds(head * HD, HD)] = value[g * tokens : (g + 1) * tokens]


def merge(state, other, copies, tokens):
    rows = state[0].shape[0]
    return pl.pallas_call(
        merge_kernel,
        out_shape=jax.ShapeDtypeStruct((copies, tokens, rows // tokens * HD), jnp.bfloat16),
        in_specs=[VMEM] * 4,
        out_specs=VMEM,
        name="merge",
        compiler_params=pltpu.CompilerParams(vmem_limit_bytes=8 * 1024 * 1024),
    )(*state, other)


def project_kernel(mine, a_ref, weight_ref, *refs):
    packs, tokens, width = a_ref.shape
    a = a_ref[...].reshape(packs * tokens, width)
    out_ref = refs[-1]
    cols = out_ref.shape[-1]
    core = lax.axis_index("core")
    for j in range(out_ref.shape[1] if mine is False else out_ref.shape[0]):
        if mine:
            at = pl.ds(pl.multiple_of((CORES * j + core) * cols, cols), cols)
            out_ref[j] = dot(a, weight_ref[:, at])
        else:
            summed = refs[0][j] + dot(a, weight_ref[j])
            out_ref[:, j] = summed.astype(jnp.bfloat16).reshape(packs, tokens, cols)


def project(a, weight, places, cols, earlier=None):
    packs, tokens, width = a.shape
    mine = earlier is None
    if mine:
        out = jax.ShapeDtypeStruct((places, packs * tokens, cols), jnp.float32)
    else:
        out = jax.ShapeDtypeStruct((packs, places, tokens, cols), jnp.bfloat16)
    args = (a, weight) if mine else (a, weight, earlier)

    def kernel(*refs):
        project_kernel(mine, *refs)

    return pl.pallas_call(
        kernel,
        out_shape=out,
        in_specs=[VMEM] * len(args),
        out_specs=VMEM,
        name="project_own" if mine else "project_other",
        cost_estimate=pl.CostEstimate(
            flops=2 * packs * tokens * width * places * cols,
            bytes_accessed=2 * width * places * cols,
            transcendentals=0,
        ),
        compiler_params=pltpu.CompilerParams(vmem_limit_bytes=16 * 1024 * 1024),
    )(*args)


def lend_kernel(weight, out_ref, sems):
    cols = out_ref.shape[2]
    theirs = 1 - lax.axis_index("core")
    copies = []
    for j in range(out_ref.shape[0]):
        at = pl.ds(pl.multiple_of((CORES * j + theirs) * cols, cols), cols)
        copies.append(pltpu.make_async_copy(weight.at[:, at], out_ref.at[j], sems.at[j]))
    for copy in copies:
        copy.start()
    for copy in copies:
        copy.wait()


def lend(weight, places, cols):
    return pl.pallas_call(
        lend_kernel,
        out_shape=jax.ShapeDtypeStruct((places, weight.shape[0], cols), weight.dtype),
        in_specs=[pl.BlockSpec(memory_space=pl.ANY)],
        out_specs=VMEM,
        scratch_shapes=[pltpu.SemaphoreType.DMA((places,))],
        name="lend",
        compiler_params=pltpu.CompilerParams(vmem_limit_bytes=8 * 1024 * 1024),
    )(weight)


def gather_sum_kernel(parts_ref, out_ref):
    packs, terms, tokens, _ = parts_ref.shape
    each = tokens // 2
    for c in range(2):
        at = pl.ds(c * each, each)
        blocks = []
        for d in range(packs):
            total = parts_ref[d, 0, at].astype(jnp.float32)
            for t in range(1, terms):
                total = total + parts_ref[d, t, at].astype(jnp.float32)
            blocks.append(total)
        out_ref[at] = jnp.stack(blocks, axis=1).astype(jnp.bfloat16)


def gather_sum(parts):
    packs, _, tokens, cols = parts.shape
    return pl.pallas_call(
        gather_sum_kernel,
        out_shape=jax.ShapeDtypeStruct((tokens, packs, cols), jnp.bfloat16),
        in_specs=[VMEM],
        out_specs=VMEM,
        name="gather_sum",
        compiler_params=pltpu.CompilerParams(vmem_limit_bytes=4 * 1024 * 1024),
    )(parts)


def local(
    queries,
    new_keys,
    new_values,
    cache_keys,
    cache_values,
    keep_lengths,
    cache_doc,
    new_doc,
    out_weight,
):
    ring = lax.axis_size("seq")
    packs, mesh_x, cores = lax.axis_size("dp"), lax.axis_size("x"), lax.axis_size("core")
    fresh = queries.shape[1]

    own, ask = pack(
        keep_lengths,
        queries[0],
        cache_keys[0],
        cache_values[0],
        new_keys[0],
        new_values[0],
        cache_doc,
        new_doc,
    )
    cols = out_weight.shape[1] // (mesh_x * cores)
    up = [(i, (i + 2) % ring) for i in range(ring)]
    down = [(i, (i - 2) % ring) for i in range(ring)]
    pair = [(i, i + 1 - 2 * (i % 2)) for i in range(ring)]
    hops = ring // 4
    state = other = None
    below = above = own
    for s in range(hops + 1):
        chunks = [below, above] if s else [own]
        if s < hops:
            if s + 1 == hops:
                below, above = below[:1], above[1:]
            below = lax.ppermute(below, "seq", up)
            above = lax.ppermute(above, "seq", down)
            if s == 0:
                asked = lax.ppermute(ask, "seq", pair)
                lent = lend(out_weight, mesh_x, cols)
                other_weight = lax.ppermute(lent, "core", [(0, 1), (1, 0)])
            state = attend(ask, chunks, state, True)
            other = attend(asked, chunks, other, False)
    (other,) = attend(asked, chunks, other, False, last=True)
    other = lax.ppermute(other, "seq", pair)
    state = attend(ask, chunks, state, True)
    attended = merge(state, other, 1, fresh)

    tiles = lax.all_gather(attended[0], "dp", axis=0)
    other_tiles = lax.ppermute(tiles, "core", [(0, 1), (1, 0)])
    part = project(tiles, out_weight, mesh_x, cols)
    pieces = project(other_tiles, other_weight, mesh_x, cols, part)
    arrived = lax.all_to_all(
        pieces.reshape(packs * mesh_x, fresh, cols), ("dp", "x"), 0, 0, tiled=True
    )
    result = gather_sum(arrived.reshape(packs, mesh_x, fresh, cols))
    return result[None]


def solution(mesh):
    shape = dict(mesh.shape)
    cores = 2
    split = Mesh(
        mesh.devices.reshape(shape["dp"], shape["seq"], shape["tensor"] // cores, cores),
        ("dp", "seq", "x", "core"),
    )
    t = ("x", "core")
    rows = P("dp", "seq", t)
    flat = P("dp", "seq")
    placed = (rows, rows, rows, rows, rows, flat, flat, flat, P(t, "dp"))

    return jax.shard_map(
        local, mesh=split, in_specs=placed, out_specs=P("dp", "seq", None, t), check_vma=False
    )
```
